128 devices in a mesh: row: 8 (over z_hi, x), col: 16 (over z_lo, y, core).
Axes of the slice: x: 4, y: 4, z: 4 (z_hi: 2, z_lo: 2; z = z_hi * 2 + z_lo), core: 2. Of those that a mesh axis runs over, the one named last changes fastest.
Arguments:
- diag_blocks: float32 [2, 512, 512], replicated, may hold values from -1 to 5, as said below
- pivot_flags: int32 [2, 512], replicated, may hold values 0 or 1
- panels: bfloat16 [2, 32768, 512], P(None, ('row', 'col')), may hold values from -3 to 3
- structure: int32 [2, 32768], P(None, ('row', 'col')), may hold values 0 or 1
- ancestor_inverse: bfloat16 [32768, 32768], P('row', 'col'), may hold values from -0.046875 to 0.046875
Outputs:
- inverse_panel: bfloat16 [2, 32768, 512], P(None, ('row', 'col'))
- inverse_diagonal: float32 [2, 512, 512], replicated
The draws below stay inside these ranges and needn't reach their ends.
Inputs may be any that keep to these rules, and one draw needn't show every extreme that they name: Each diag_blocks[k] is symmetric, and its off-diagonal part is small enough that every eigenvalue of each shifted block is at least 0.8, so every shifted block is positive definite.
All inputs are finite; a program needn't handle non-finite values. No bound on the sum of `structure` on one device may be relied on, other than what follows from the above.
Results may differ from the reference program's by a relative error of at most 0.0051.
Values may be sent and summed in bfloat16 or wider, within the bound.
No kernel may reach another device: no remote copies, remote signals or barrier semaphores. Data moves between devices by JAX's collectives and lax.ppermute only.
A program may use at most 192 MiB of HBM per device.

```python
import math
import jax
import jax.numpy as jnp
from jax import lax

W = 512
NODES = 2
R = 32768
N_ROW = 8


def draw_diag_blocks(key, part):
    key_off, key_diag = jax.random.split(jax.random.fold_in(key, 11))
    spread_off = 0.6
    lower_end = 2.0
    upper_end = 4.0
    noise_term = jax.random.normal(key_off, (NODES, W, W), jnp.float32) * (spread_off / math.sqrt(W))
    symmetric = (noise_term + jnp.swapaxes(noise_term, 1, 2)) / math.sqrt(2.0)
    identity = jnp.eye(W, dtype=jnp.float32)
    symmetric = symmetric * (1.0 - identity)[None, :, :]
    diagonal = jax.random.uniform(key_diag, (NODES, W), jnp.float32, lower_end, upper_end)
    return symmetric + identity[None, :, :] * diagonal[:, None, :]


def touch_ends(entries, stream_key, low, high):
    dims = entries.shape
    spot = [jax.random.randint(jax.random.fold_in(stream_key, axis), (), 0, dims[axis]) for axis in range(len(dims))]
    entries = entries.at[tuple(spot)].set(low)
    longest = dims.index(max(dims))
    spot[longest] = (spot[longest] + 1) % dims[longest]
    return entries.at[tuple(spot)].set(high)


def raised(result, stream_key, source, target, parts, factor):
    owner, partner = [(jnp.arange(result.shape[position]) // (result.shape[position] // parts)).reshape([-1 if axis == position else 1 for axis in range(result.ndim)]) for position in (source, target)]
    chosen = jax.random.permutation(stream_key, parts)[partner]
    strong = (owner == chosen) | (owner == (partner + parts // 2) % parts)
    return jnp.where(strong, factor * result, result)


def shard_levels(stream_key, extent, pieces, smallest, top_value):
    factor_of = 1.0
    for dim, blocks in pieces:
        heights = jax.random.uniform(jax.random.fold_in(jax.random.fold_in(stream_key, 6), dim), (blocks,), jnp.float32, smallest / len(pieces), top_value / len(pieces))
        factor_of = factor_of * jnp.repeat(jnp.exp(heights), extent[dim] // blocks).reshape((-1,) + (1,) * (len(extent) - 1 - dim))
    return factor_of


def noise(rng, extent, scale, limit, shards=(), kind=jnp.bfloat16):
    loudness = shard_levels(rng, extent, shards, -0.22, 0.18) if shards else 1.0
    drawn = jax.random.normal(rng, extent, jnp.float32) * scale * loudness
    return jnp.minimum(jnp.maximum(drawn, -limit), limit).astype(kind)


def noise_with(key, extent, width, bound, pieces, heavy, held_as=jnp.bfloat16):
    values = width * jax.random.normal(key, extent, jnp.float32)
    if pieces:
        values = values * shard_levels(key, extent, pieces, -0.22, 0.18)
    return jnp.clip(raised(values, jax.random.fold_in(key, 3), *heavy), -bound, bound).astype(held_as)


def setup_inputs(seed: int = 0) -> dict:
    seeds = jax.random.split(jax.random.key(seed), 6)
    return {
        "diag_blocks": draw_diag_blocks(jax.random.fold_in(seeds[5], 71), 0),
        "pivot_flags": touch_ends((jax.random.randint(seeds[1], (NODES, W), 0, 4) < 1).astype(jnp.int32), jax.random.fold_in(seeds[1], 1), 0, 1),
        "panels": noise(seeds[2], (NODES, R, W), 0.5, 3.0, ((1, 128),)),
        "structure": touch_ends((jax.random.randint(seeds[3], (NODES, R), 0, 4) < 3).astype(jnp.int32), jax.random.fold_in(seeds[3], 1), 0, 1),
        "ancestor_inverse": noise_with(seeds[4], (R, R), R ** -0.5, 0.046875, ((0, 8), (1, 16)), (1, 0, 16, 2.0)),
    }


HIGHEST_PRECISION = lax.Precision.HIGHEST
PERTURBATION = 1.0

def factor_inverse(diagonal_block, flag_row):
    node_width = diagonal_block.shape[0]
    identity = jnp.eye(node_width, dtype=jnp.float32)
    shifted = diagonal_block + PERTURBATION * identity * flag_row.astype(jnp.float32)[None, :]
    factor_lower = jnp.linalg.cholesky(shifted)
    lower_inverse = jax.scipy.linalg.solve_triangular(factor_lower, identity, lower=True)
    return jnp.dot(lower_inverse.T, lower_inverse, precision=HIGHEST_PRECISION)

def normalize_panel(panel_rows, member_row, inverse):
    masked = panel_rows.astype(jnp.float32) * member_row.astype(jnp.float32)[:, None]
    return jnp.dot(masked, inverse, precision=HIGHEST_PRECISION).astype(jnp.bfloat16)

def reference(diag_blocks, pivot_flags, panels, structure, ancestor_inverse):
    matrix_order = ancestor_inverse.shape[0]
    tile_rows = matrix_order // N_ROW
    blocks = ancestor_inverse.reshape(N_ROW, tile_rows, matrix_order)
    panel_list = []
    diagonal_list = []
    for supernode in range(diag_blocks.shape[0]):
        inverse = factor_inverse(diag_blocks[supernode], pivot_flags[supernode])
        normed = normalize_panel(panels[supernode], structure[supernode], inverse)
        normed_wide = normed.astype(jnp.float32)

        def product(block_rows):
            return jnp.dot(block_rows.astype(jnp.float32), normed_wide, precision=HIGHEST_PRECISION)
        applied = lax.map(product, blocks).reshape(matrix_order, normed.shape[1])
        panel_list.append((-applied).astype(jnp.bfloat16))
        diagonal_list.append(inverse + jnp.dot(normed_wide.T, applied, precision=HIGHEST_PRECISION))
    return (jnp.stack(panel_list), jnp.stack(diagonal_list))
```

```python
import functools

import jax
import jax.numpy as jnp
import numpy as np
from jax import lax
from jax.experimental import pallas as pl
from jax.experimental.pallas import tpu as pltpu
from jax.sharding import Mesh, PartitionSpec as P

HIGHEST = lax.Precision.HIGHEST
PERTURBATION = 1.0
BLOCK = 128
STRIP = 8
GROUP = 2
ROW = ("z_hi", "x")
COL = ("z_lo", "y", "core")
AXES = ROW + COL
CHIPS = ("z_hi", "x", "z_lo", "y")
MESH_SHAPE = (2, 4, 2, 4, 2)


def after(value, *earlier):
    return lax.optimization_barrier((value, earlier))[0]


def lane_spread(tile, lane):
    index = jnp.full(tile.shape, lane, jnp.int32)
    return jnp.take_along_axis(tile, index, axis=1, mode="promise_in_bounds")


def small_inverses(nodes):
    row = lax.broadcasted_iota(jnp.int32, nodes[0][0].shape, 0)
    for i in range(len(nodes[0])):
        at = row == i
        pivot = [1.0 / cols[i][i : i + 1, :] for cols in nodes]
        left = [jnp.where(at, -1.0, cols[i]) for cols in nodes]
        nodes = [
            [
                -l * p if j == i else jnp.where(at, 0.0, cols[j]) - l * (cols[j][i : i + 1, :] * p)
                for j in range(len(cols))
            ]
            for cols, l, p in zip(nodes, left, pivot)
        ]
    return nodes


def invert_blocks(ref):
    count, n, _ = ref.shape
    nodes = range(count)
    lane = lax.broadcasted_iota(jnp.int32, (STRIP, n), 1)
    wide = lax.broadcasted_iota(jnp.int32, (n, n), 1)

    def step(strip, carry):
        base = pl.multiple_of(strip * STRIP, STRIP)
        inside = (wide >= base) & (wide < base + STRIP)
        whole = [ref[k] for k in nodes]
        rows = [ref[k, pl.ds(base, STRIP), :] for k in nodes]
        small = small_inverses(
            [[lane_spread(rows[k], base + j) for j in range(STRIP)] for k in nodes]
        )
        top = [small[k][0] * rows[k][0:1, :] for k in nodes]
        for j in range(1, STRIP):
            top = [top[k] + small[k][j] * rows[k][j : j + 1, :] for k in nodes]
        for j in range(STRIP):
            top = [jnp.where(lane == base + j, small[k][j], top[k]) for k in nodes]
        rest = [jnp.where(inside, 0.0, whole[k]) for k in nodes]
        for j in range(STRIP):
            rest = [
                rest[k] - lane_spread(whole[k], base + j) * top[k][j : j + 1, :] for k in nodes
            ]
        for k in nodes:
            ref[k] = rest[k]
            ref[k, pl.ds(base, STRIP), :] = top[k]
        return carry

    lax.fori_loop(0, n // STRIP, step, 0)


def inverse_kernel(block, in_ref, flag_ref, out_ref, block_ref, panel_ref):
    count, width, _ = in_ref.shape
    n = block_ref.shape[1]
    here = pl.ds(block * n, n)
    if block == 0:
        row = lax.broadcasted_iota(jnp.int32, (width, width), 0)
        col = lax.broadcasted_iota(jnp.int32, (width, width), 1)
        for k in range(count):
            shifts = PERTURBATION * flag_ref[k : k + 1, :].astype(jnp.float32)
            out_ref[k] = in_ref[k] + jnp.where(row == col, shifts, 0.0)
    else:
        out_ref[...] = in_ref[...]
    for k in range(count):
        block_ref[k] = out_ref[k, here, here]
    invert_blocks(block_ref)

    def update(k, carry):
        inner = block_ref[k]
        panel_ref[...] = jnp.dot(
            inner, out_ref[k, here, :], precision=HIGHEST, preferred_element_type=jnp.float32
        )
        panel_ref[:, here] = inner
        left = out_ref[k, :, here]
        out_ref[k, :, here] = jnp.zeros((width, n), jnp.float32)
        out_ref[k] = out_ref[k] - jnp.dot(
            left, panel_ref[...], precision=HIGHEST, preferred_element_type=jnp.float32
        )
        out_ref[k, here, :] = panel_ref[...]
        return carry

    lax.fori_loop(0, count, update, 0)


def eliminate(block, matrices, pivot_flags):
    count, width, _ = matrices.shape
    return pl.pallas_call(
        functools.partial(inverse_kernel, block),
        out_shape=jax.ShapeDtypeStruct(matrices.shape, jnp.float32),
        scratch_shapes=[
            pltpu.VMEM((count, BLOCK, BLOCK), jnp.float32),
            pltpu.VMEM((BLOCK, width), jnp.float32),
        ],
        compiler_params=pltpu.CompilerParams(vmem_limit_bytes=32 * 2**20),
        cost_estimate=pl.CostEstimate(
            flops=5 * 10**9, bytes_accessed=8 * matrices.size, transcendentals=0
        ),
        name="eliminate",
    )(matrices, pivot_flags)


def shift(value, **steps):
    return send(value, lambda **at: {name: at[name] + by for name, by in steps.items()})


def send(value, target):
    extents = [lax.axis_size(name) for name in AXES]
    moves = []
    for source in np.ndindex(*extents):
        at = {name: int(i) for name, i in zip(AXES, source)}
        at.update(target(**at))
        there = [at[name] % extent for name, extent in zip(AXES, extents)]
        moves.append(tuple(int(np.ravel_multi_index(i, extents)) for i in (source, there)))
    return lax.ppermute(value, AXES, moves)


def seed(strip, flip):
    return send(
        strip,
        lambda z_hi, x, z_lo, y, core: dict(
            z_hi=y // 2 ^ flip, x=y % 2 * 2 + core, z_lo=z_hi, y=x, core=z_lo
        ),
    )


def product_kernel(order_ref, place_ref, *refs):
    tiles, (*pieces, out_ref, columns_ref) = refs[:GROUP], refs[GROUP:]
    rows = pieces[0].shape[1]

    @pl.when(pl.program_id(0) == 0)
    def _():
        slot = 0
        for piece in pieces:
            for part in range(piece.shape[0]):
                start = pl.multiple_of(place_ref[slot] * rows, rows)
                columns_ref[pl.ds(start, rows), :] = piece[part]
                slot += 1

    tile = jnp.concatenate([ref[0] for ref in tiles], axis=0)
    out = jnp.dot(tile, columns_ref[...], preferred_element_type=jnp.float32)
    out_ref[...] = out.astype(out_ref.dtype).reshape(out_ref.shape)


def product(tile, pieces, order, place, dtype):
    blocks = order.shape[0]
    _, rows, depth = tile.shape
    width = pieces[0].shape[2]

    def tile_spec(member):
        return pl.BlockSpec(
            (1, rows, depth), lambda i, order, place: (order[GROUP * i + member], 0, 0)
        )

    return pl.pallas_call(
        product_kernel,
        out_shape=jax.ShapeDtypeStruct((blocks, rows, width), dtype),
        grid_spec=pltpu.PrefetchScalarGridSpec(
            num_scalar_prefetch=2,
            grid=(blocks // GROUP,),
            in_specs=[tile_spec(member) for member in range(GROUP)]
            + [pl.BlockSpec(p.shape, lambda i, order, place: (0, 0, 0)) for p in pieces],
            out_specs=pl.BlockSpec((GROUP, rows, width), lambda i, order, place: (i, 0, 0)),
            scratch_shapes=[pltpu.VMEM((depth, width), jnp.bfloat16)],
        ),
        compiler_params=pltpu.CompilerParams(vmem_limit_bytes=60 * 2**20),
        cost_estimate=pl.CostEstimate(
            flops=2 * blocks * rows * depth * width,
            bytes_accessed=2 * blocks * rows * depth + 2 * depth * width,
            transcendentals=0,
        ),
        name="product",
    )(order, place, *[tile] * GROUP, *pieces)


def total(term):
    core = lax.axis_index("core")
    half = term.shape[0] // 2
    chips = 64
    low, high = term[:half], term[half:]
    part = jnp.where(core == 0, low, high) + shift(jnp.where(core == 0, high, low), core=1)
    slices = lax.all_to_all(part.reshape(chips, half // chips, -1), CHIPS, 0, 0)
    summed = jnp.sum(slices, axis=0, keepdims=True).astype(jnp.bfloat16)
    spread = lax.all_to_all(jnp.broadcast_to(summed, slices.shape), CHIPS, 0, 0)
    own = spread.reshape(half, -1)
    other = shift(own, core=1)
    return jnp.concatenate([jnp.where(core == 0, own, other), jnp.where(core == 0, other, own)])


def invert(diag_blocks, pivot_flags, panels, structure, ancestor_inverse):
    nodes, own_rows, _ = panels.shape
    z_hi, x, z_lo, y, core = [lax.axis_index(name) for name in AXES]
    tile = ancestor_inverse.reshape(16, own_rows, ancestor_inverse.shape[1])
    masked = [
        jnp.where(structure[k][:, None] != 0, panels[k], 0).astype(jnp.bfloat16)
        for k in range(nodes)
    ]
    steps = [(d, e) for d in range(4) for e in range(2)]
    kept = jnp.stack([(z_lo ^ e) * 8 + (y + d) % 4 * 2 + core for d, e in steps]).astype(jnp.int32)

    seeds = [seed(masked[0], flip) for flip in range(2)]
    along = [masked[1]] + [shift(masked[1], x=d) for d in (1, 2, 3)]

    state = eliminate(0, diag_blocks, pivot_flags)
    state = eliminate(1, state, pivot_flags)

    pair = after(jnp.stack(seeds), state)
    first = [pair] + [shift(pair, x=d) for d in (1, 2, 3)]
    first_place = jnp.stack([(z_hi ^ e) * 4 + (x - d) % 4 for d, e in steps]).astype(jnp.int32)

    stacked = after(jnp.stack(along), state)
    turned = []
    for d in range(4):
        part = lax.dynamic_index_in_dim(stacked, (x - y - d) % 4, 0, keepdims=False)
        turned.append(shift(part, y=d) if d else part)

    state = eliminate(2, after(state, pair, stacked), pivot_flags)
    quad = after(jnp.stack(turned), state)
    second = []
    for flip in range(2):
        second.append(
            send(quad, lambda z_hi, x, z_lo, y, core: dict(z_hi=core ^ flip, z_lo=z_hi, core=z_lo))
        )
    second_place = jnp.stack(
        [(y - d) % 4 * 2 + (z_hi ^ flip) for flip in range(2) for d in range(4)]
    ).astype(jnp.int32)
    inverses = eliminate(3, after(state, quad), pivot_flags)

    pieces = [first, second]
    places = [first_place, second_place]
    order = after(kept, inverses)
    applied, terms = [], []
    for k in range(nodes):
        given = product(tile, pieces[k], order ^ 1, places[k], jnp.bfloat16)
        other = shift(given, core=1)
        mine = product(tile, pieces[k], order, places[k], jnp.float32)
        both = mine + other.astype(jnp.float32)
        leaving = [both[2 * d : 2 * d + 2].astype(jnp.bfloat16) for d in (1, 2, 3)]
        order = after(kept, *leaving)
        summed = both[0:2]
        for d, part in zip((1, 2, 3), leaving):
            arrived = shift(part, y=d)
            summed = summed + arrived.astype(jnp.float32)
        summed = summed[0] + shift(summed[1].astype(jnp.bfloat16), z_lo=1).astype(jnp.float32)
        applied.append(jnp.dot(summed, inverses[k], precision=HIGHEST))
        normed = jnp.dot(masked[k].astype(jnp.float32), inverses[k], precision=HIGHEST)
        terms.append(
            lax.dot_general(
                normed.astype(jnp.bfloat16).astype(jnp.float32),
                applied[k],
                (((0,), (0,)), ((), ())),
                precision=HIGHEST,
                preferred_element_type=jnp.float32,
            )
        )
        last = leaving
    totals = [total(after(terms[0], *last)), total(terms[1])]
    inverse_diagonal = jnp.stack(
        [inverses[k] + totals[k].astype(jnp.float32) for k in range(nodes)]
    )
    inverse_panel = (-jnp.stack(applied)).astype(jnp.bfloat16)
    return (inverse_panel, inverse_diagonal)


def solution(mesh):
    mesh = Mesh(mesh.devices.reshape(MESH_SHAPE), AXES)
    in_specs = (P(), P(), P(None, AXES, None), P(None, AXES), P(ROW, COL))
    out_specs = (P(None, AXES, None), P())
    return jax.shard_map(invert, mesh=mesh, in_specs=in_specs, out_specs=out_specs, check_vma=False)
```

```python
import functools

import jax
import jax.numpy as jnp
import numpy as np
from jax import lax
from jax.experimental import pallas as pl
from jax.experimental.pallas import tpu as pltpu
from jax.sharding import Mesh, PartitionSpec as P

HIGHEST = lax.Precision.HIGHEST
PERTURBATION = 1.0
BLOCK = 128
STRIP = 8
GROUP = 2
ROW = ("z_hi", "x")
COL = ("z_lo", "y", "core")
AXES = ROW + COL
CHIPS = ("z_hi", "x", "z_lo", "y")
MESH_SHAPE = (2, 4, 2, 4, 2)


def after(value, *earlier):
    return lax.optimization_barrier((value, earlier))[0]


def lane_spread(tile, lane):
    index = jnp.full(tile.shape, lane, jnp.int32)
    return jnp.take_along_axis(tile, index, axis=1, mode="promise_in_bounds")


def small_inverses(nodes):
    row = lax.broadcasted_iota(jnp.int32, nodes[0][0].shape, 0)
    for i in range(len(nodes[0])):
        at = row == i
        pivot = [1.0 / cols[i][i : i + 1, :] for cols in nodes]
        left = [jnp.where(at, -1.0, cols[i]) for cols in nodes]
        nodes = [
            [
                -l * p if j == i else jnp.where(at, 0.0, cols[j]) - l * (cols[j][i : i + 1, :] * p)
                for j in range(len(cols))
            ]
            for cols, l, p in zip(nodes, left, pivot)
        ]
    return nodes


def invert_blocks(ref):
    count, n, _ = ref.shape
    nodes = range(count)
    lane = lax.broadcasted_iota(jnp.int32, (STRIP, n), 1)
    wide = lax.broadcasted_iota(jnp.int32, (n, n), 1)

    def step(strip, carry):
        base = pl.multiple_of(strip * STRIP, STRIP)
        inside = (wide >= base) & (wide < base + STRIP)
        whole = [ref[k] for k in nodes]
        rows = [ref[k, pl.ds(base, STRIP), :] for k in nodes]
        small = small_inverses(
            [[lane_spread(rows[k], base + j) for j in range(STRIP)] for k in nodes]
        )
        top = [small[k][0] * rows[k][0:1, :] for k in nodes]
        for j in range(1, STRIP):
            top = [top[k] + small[k][j] * rows[k][j : j + 1, :] for k in nodes]
        for j in range(STRIP):
            top = [jnp.where(lane == base + j, small[k][j], top[k]) for k in nodes]
        rest = [jnp.where(inside, 0.0, whole[k]) for k in nodes]
        for j in range(STRIP):
            rest = [
                rest[k] - lane_spread(whole[k], base + j) * top[k][j : j + 1, :] for k in nodes
            ]
        for k in nodes:
            ref[k] = rest[k]
            ref[k, pl.ds(base, STRIP), :] = top[k]
        return carry

    lax.fori_loop(0, n // STRIP, step, 0)


def inverse_kernel(block, in_ref, flag_ref, out_ref, block_ref, panel_ref):
    count, width, _ = in_ref.shape
    n = block_ref.shape[1]
    here = pl.ds(block * n, n)
    if block == 0:
        row = lax.broadcasted_iota(jnp.int32, (width, width), 0)
        col = lax.broadcasted_iota(jnp.int32, (width, width), 1)
        for k in range(count):
            shifts = PERTURBATION * flag_ref[k : k + 1, :].astype(jnp.float32)
            out_ref[k] = in_ref[k] + jnp.where(row == col, shifts, 0.0)
    else:
        out_ref[...] = in_ref[...]
    for k in range(count):
        block_ref[k] = out_ref[k, here, here]
    invert_blocks(block_ref)

    def update(k, carry):
        inner = block_ref[k]
        panel_ref[...] = jnp.dot(
            inner, out_ref[k, here, :], precision=HIGHEST, preferred_element_type=jnp.float32
        )
        panel_ref[:, here] = inner
        left = out_ref[k, :, here]
        out_ref[k, :, here] = jnp.zeros((width, n), jnp.float32)
        out_ref[k] = out_ref[k] - jnp.dot(
            left, panel_ref[...], precision=HIGHEST, preferred_element_type=jnp.float32
        )
        out_ref[k, here, :] = panel_ref[...]
        return carry

    lax.fori_loop(0, count, update, 0)


def eliminate(block, matrices, pivot_flags):
    count, width, _ = matrices.shape
    return pl.pallas_call(
        functools.partial(inverse_kernel, block),
        out_shape=jax.ShapeDtypeStruct(matrices.shape, jnp.float32),
        scratch_shapes=[
            pltpu.VMEM((count, BLOCK, BLOCK), jnp.float32),
            pltpu.VMEM((BLOCK, width), jnp.float32),
        ],
        compiler_params=pltpu.CompilerParams(vmem_limit_bytes=32 * 2**20),
        cost_estimate=pl.CostEstimate(
            flops=5 * 10**9, bytes_accessed=8 * matrices.size, transcendentals=0
        ),
        name="eliminate",
    )(matrices, pivot_flags)


def shift(value, **steps):
    return send(value, lambda **at: {name: at[name] + by for name, by in steps.items()})


def send(value, target):
    extents = [lax.axis_size(name) for name in AXES]
    moves = []
    for source in np.ndindex(*extents):
        at = {name: int(i) for name, i in zip(AXES, source)}
        at.update(target(**at))
        there = [at[name] % extent for name, extent in zip(AXES, extents)]
        moves.append(tuple(int(np.ravel_multi_index(i, extents)) for i in (source, there)))
    return lax.ppermute(value, AXES, moves)


def seed(strip, flip):
    return send(
        strip,
        lambda z_hi, x, z_lo, y, core: dict(
            z_hi=y // 2 ^ flip, x=y % 2 * 2 + core, z_lo=z_hi, y=x, core=z_lo
        ),
    )


def fill_columns(place_ref, pieces, columns_ref):
    rows = pieces[0].shape[1]

    @pl.when(pl.program_id(0) == 0)
    def _():
        slot = 0
        for piece in pieces:
            for part in range(piece.shape[0]):
                start = pl.multiple_of(place_ref[slot] * rows, rows)
                columns_ref[pl.ds(start, rows), :] = piece[part]
                slot += 1


def tile_product(tiles, columns_ref):
    tile = jnp.concatenate([ref[0] for ref in tiles], axis=0)
    out = jnp.dot(tile, columns_ref[...], preferred_element_type=jnp.float32)
    return out.reshape(GROUP, -1, out.shape[1])


def given_kernel(order_ref, place_ref, *refs):
    tiles, (*pieces, out_ref, columns_ref) = refs[:GROUP], refs[GROUP:]
    fill_columns(place_ref, pieces, columns_ref)
    out_ref[...] = tile_product(tiles, columns_ref).astype(out_ref.dtype)


def mine_kernel(order_ref, place_ref, *refs):
    tiles, (*pieces, other_ref, o0, o1, o2, o3, columns_ref) = refs[:GROUP], refs[GROUP:]
    fill_columns(place_ref, pieces, columns_ref)
    both = tile_product(tiles, columns_ref) + other_ref[...].astype(jnp.float32)
    for d, out_ref in enumerate((o0, o1, o2, o3)):

        @pl.when(pl.program_id(0) == d)
        def _(out_ref=out_ref):
            out_ref[...] = both.astype(out_ref.dtype)


def product(tile, pieces, order, place, other=None):
    blocks = order.shape[0]
    _, rows, depth = tile.shape
    width = pieces[0].shape[2]

    def tile_spec(member):
        return pl.BlockSpec(
            (1, rows, depth), lambda i, order, place: (order[GROUP * i + member], 0, 0)
        )

    whole = lambda i, order, place: (0, 0, 0)
    step = pl.BlockSpec((GROUP, rows, width), lambda i, order, place: (i, 0, 0))
    in_specs = [tile_spec(member) for member in range(GROUP)]
    in_specs += [pl.BlockSpec(p.shape, whole) for p in pieces]
    operands = [tile] * GROUP + list(pieces)
    if other is None:
        kernel, out_specs = given_kernel, step
        out_shape = jax.ShapeDtypeStruct((blocks, rows, width), jnp.bfloat16)
    else:
        kernel, out_specs = mine_kernel, [pl.BlockSpec((GROUP, rows, width), whole)] * 4
        out_shape = [
            jax.ShapeDtypeStruct((GROUP, rows, width), dtype)
            for dtype in (jnp.float32, jnp.bfloat16, jnp.bfloat16, jnp.bfloat16)
        ]
        in_specs.append(step)
        operands.append(other)
    return pl.pallas_call(
        kernel,
        out_shape=out_shape,
        grid_spec=pltpu.PrefetchScalarGridSpec(
            num_scalar_prefetch=2,
            grid=(blocks // GROUP,),
            in_specs=in_specs,
            out_specs=out_specs,
            scratch_shapes=[pltpu.VMEM((depth, width), jnp.bfloat16)],
        ),
        compiler_params=pltpu.CompilerParams(vmem_limit_bytes=50 * 2**20),
        cost_estimate=pl.CostEstimate(
            flops=2 * blocks * rows * depth * width,
            bytes_accessed=2 * blocks * rows * depth + 2 * depth * width,
            transcendentals=0,
        ),
        name="product",
    )(order, place, *operands)


def total(term):
    core = lax.axis_index("core")
    half = term.shape[0] // 2
    chips = 64
    low, high = term[:half], term[half:]
    part = jnp.where(core == 0, low, high) + shift(jnp.where(core == 0, high, low), core=1)
    slices = part.astype(jnp.bfloat16).reshape(chips, half // chips, -1)
    slices = lax.all_to_all(slices, CHIPS, 0, 0)
    summed = jnp.sum(slices.astype(jnp.float32), axis=0, keepdims=True).astype(jnp.bfloat16)
    spread = lax.all_to_all(jnp.broadcast_to(summed, slices.shape), CHIPS, 0, 0)
    own = spread.reshape(half, -1)
    other = shift(own, core=1)
    return jnp.concatenate([jnp.where(core == 0, own, other), jnp.where(core == 0, other, own)])


def invert(diag_blocks, pivot_flags, panels, structure, ancestor_inverse):
    nodes, own_rows, _ = panels.shape
    z_hi, x, z_lo, y, core = [lax.axis_index(name) for name in AXES]
    tile = ancestor_inverse.reshape(16, own_rows, ancestor_inverse.shape[1])
    masked = [
        jnp.where(structure[k][:, None] != 0, panels[k], 0).astype(jnp.bfloat16)
        for k in range(nodes)
    ]
    steps = [(d, e) for d in range(4) for e in range(2)]
    kept = jnp.stack([(z_lo ^ e) * 8 + (y + d) % 4 * 2 + core for d, e in steps]).astype(jnp.int32)

    seeds = []
    for flip in range(2):
        seeds.append(seed(masked[0], flip))
    crossed = send(
        masked[1], lambda z_hi, x, z_lo, y, core: dict(z_hi=z_lo, z_lo=z_hi)
    )
    along = [crossed]
    for d in (1, 2, 3):
        along.append(shift(crossed, x=d))

    state = eliminate(0, diag_blocks, pivot_flags)

    pair = after(jnp.stack(seeds), state)
    first = [pair]
    for d in (1, 2, 3):
        first.append(shift(pair, x=d))
    first_place = jnp.stack([(z_hi ^ e) * 4 + (x - d) % 4 for d, e in steps]).astype(jnp.int32)

    stacked = after(jnp.stack(along), pair)
    turned = []
    for d in range(4):
        part = lax.dynamic_index_in_dim(stacked, (x - y - d) % 4, 0, keepdims=False)
        turned.append(shift(part, y=d) if d else part)

    state = eliminate(1, after(state, pair, stacked), pivot_flags)
    quad = after(jnp.stack(turned), state)
    second = []
    for flip in range(2):
        second.append(
            send(
                quad,
                lambda z_hi, x, z_lo, y, core: dict(z_hi=core ^ flip, core=z_hi),
            )
        )
    second_place = jnp.stack(
        [(y - d) % 4 * 2 + (z_hi ^ flip) for flip in range(2) for d in range(4)]
    ).astype(jnp.int32)

    pieces = [first, second]
    places = [first_place, second_place]
    swapped = []
    order = after(kept, quad)
    for k in range(nodes):
        given = product(tile, pieces[k], order ^ 1, places[k])
        swapped.append(shift(given, core=1))
        order = after(kept, given)
    sums = []
    for k in range(nodes):
        staying, *leaving = product(tile, pieces[k], order, places[k], swapped[k])
        order = after(kept, *leaving)
        summed = staying
        for d, part in zip((1, 2, 3), leaving):
            arrived = shift(part, y=d)
            summed = summed + arrived.astype(jnp.float32)
        arrived = shift(summed[1].astype(jnp.bfloat16), z_lo=1)
        sums.append(summed[0] + arrived.astype(jnp.float32))

    state = eliminate(2, after(state, *leaving), pivot_flags)
    inverses = eliminate(3, state, pivot_flags)
    applied, terms = [], []
    for k in range(nodes):
        applied.append(jnp.dot(sums[k], inverses[k], precision=HIGHEST))
        normed = jnp.dot(masked[k].astype(jnp.float32), inverses[k], precision=HIGHEST)
        terms.append(
            lax.dot_general(
                normed.astype(jnp.bfloat16).astype(jnp.float32),
                applied[k],
                (((0,), (0,)), ((), ())),
                precision=HIGHEST,
                preferred_element_type=jnp.float32,
            )
        )
    totals = total(jnp.concatenate(terms)).astype(jnp.float32).reshape(inverses.shape)
    inverse_diagonal = inverses + totals
    inverse_panel = (-jnp.stack(applied)).astype(jnp.bfloat16)
    return (inverse_panel, inverse_diagonal)


def solution(mesh):
    mesh = Mesh(mesh.devices.reshape(MESH_SHAPE), AXES)
    in_specs = (P(), P(), P(None, AXES, None), P(None, AXES), P(ROW, COL))
    out_specs = (P(None, AXES, None), P())
    return jax.shard_map(invert, mesh=mesh, in_specs=in_specs, out_specs=out_specs, check_vma=False)
```

```python
import functools

import jax
import jax.numpy as jnp
import numpy as np
from jax import lax
from jax.experimental import pallas as pl
from jax.experimental.pallas import tpu as pltpu
from jax.sharding import Mesh, PartitionSpec as P

HIGHEST = lax.Precision.HIGHEST
PERTURBATION = 1.0
BLOCK = 128
STRIP = 8
GROUP = 2
ROW = ("z_hi", "x")
COL = ("z_lo", "y", "core")
AXES = ROW + COL
CHIPS = ("z_hi", "x", "z_lo", "y")
MESH_SHAPE = (2, 4, 2, 4, 2)


def after(value, *earlier):
    return lax.optimization_barrier((value, earlier))[0]


def lane_spread(tile, lane):
    index = jnp.full(tile.shape, lane, jnp.int32)
    return jnp.take_along_axis(tile, index, axis=1, mode="promise_in_bounds")


def small_inverses(nodes):
    row = lax.broadcasted_iota(jnp.int32, nodes[0][0].shape, 0)
    for i in range(len(nodes[0])):
        at = row == i
        pivot = [1.0 / cols[i][i : i + 1, :] for cols in nodes]
        left = [jnp.where(at, -1.0, cols[i]) for cols in nodes]
        nodes = [
            [
                -l * p if j == i else jnp.where(at, 0.0, cols[j]) - l * (cols[j][i : i + 1, :] * p)
                for j in range(len(cols))
            ]
            for cols, l, p in zip(nodes, left, pivot)
        ]
    return nodes


def invert_blocks(ref):
    count, n, _ = ref.shape
    nodes = range(count)
    lane = lax.broadcasted_iota(jnp.int32, (STRIP, n), 1)
    wide = lax.broadcasted_iota(jnp.int32, (n, n), 1)

    def step(strip, carry):
        base = pl.multiple_of(strip * STRIP, STRIP)
        inside = (wide >= base) & (wide < base + STRIP)
        whole = [ref[k] for k in nodes]
        rows = [ref[k, pl.ds(base, STRIP), :] for k in nodes]
        small = small_inverses(
            [[lane_spread(rows[k], base + j) for j in range(STRIP)] for k in nodes]
        )
        top = [small[k][0] * rows[k][0:1, :] for k in nodes]
        for j in range(1, STRIP):
            top = [top[k] + small[k][j] * rows[k][j : j + 1, :] for k in nodes]
        for j in range(STRIP):
            top = [jnp.where(lane == base + j, small[k][j], top[k]) for k in nodes]
        rest = [jnp.where(inside, 0.0, whole[k]) for k in nodes]
        for j in range(STRIP):
            rest = [
                rest[k] - lane_spread(whole[k], base + j) * top[k][j : j + 1, :] for k in nodes
            ]
        for k in nodes:
            ref[k] = rest[k]
            ref[k, pl.ds(base, STRIP), :] = top[k]
        return carry

    lax.fori_loop(0, n // STRIP, step, 0)


def inverse_kernel(block, in_ref, flag_ref, out_ref, block_ref, panel_ref):
    count, width, _ = in_ref.shape
    n = block_ref.shape[1]
    here = pl.ds(block * n, n)
    if block == 0:
        row = lax.broadcasted_iota(jnp.int32, (width, width), 0)
        col = lax.broadcasted_iota(jnp.int32, (width, width), 1)
        for k in range(count):
            shifts = PERTURBATION * flag_ref[k : k + 1, :].astype(jnp.float32)
            out_ref[k] = in_ref[k] + jnp.where(row == col, shifts, 0.0)
    else:
        out_ref[...] = in_ref[...]
    for k in range(count):
        block_ref[k] = out_ref[k, here, here]
    invert_blocks(block_ref)

    def update(k, carry):
        inner = block_ref[k]
        panel_ref[...] = jnp.dot(
            inner, out_ref[k, here, :], precision=HIGHEST, preferred_element_type=jnp.float32
        )
        panel_ref[:, here] = inner
        left = out_ref[k, :, here]
        out_ref[k, :, here] = jnp.zeros((width, n), jnp.float32)
        out_ref[k] = out_ref[k] - jnp.dot(
            left, panel_ref[...], precision=HIGHEST, preferred_element_type=jnp.float32
        )
        out_ref[k, here, :] = panel_ref[...]
        return carry

    lax.fori_loop(0, count, update, 0)


def eliminate(block, matrices, pivot_flags):
    count, width, _ = matrices.shape
    return pl.pallas_call(
        functools.partial(inverse_kernel, block),
        out_shape=jax.ShapeDtypeStruct(matrices.shape, jnp.float32),
        scratch_shapes=[
            pltpu.VMEM((count, BLOCK, BLOCK), jnp.float32),
            pltpu.VMEM((BLOCK, width), jnp.float32),
        ],
        compiler_params=pltpu.CompilerParams(vmem_limit_bytes=32 * 2**20),
        cost_estimate=pl.CostEstimate(
            flops=5 * 10**9, bytes_accessed=8 * matrices.size, transcendentals=0
        ),
        name="eliminate",
    )(matrices, pivot_flags)


def shift(value, **steps):
    return send(value, lambda **at: {name: at[name] + by for name, by in steps.items()})


def send(value, target):
    extents = [lax.axis_size(name) for name in AXES]
    moves = []
    for source in np.ndindex(*extents):
        at = {name: int(i) for name, i in zip(AXES, source)}
        at.update(target(**at))
        there = [at[name] % extent for name, extent in zip(AXES, extents)]
        moves.append(tuple(int(np.ravel_multi_index(i, extents)) for i in (source, there)))
    return lax.ppermute(value, AXES, moves)


def seed(strip, flip):
    return send(
        strip,
        lambda z_hi, x, z_lo, y, core: dict(
            z_hi=y // 2 ^ flip, x=y % 2 * 2 + core, z_lo=z_hi, y=x, core=z_lo
        ),
    )


def fill_columns(place_ref, pieces, columns_ref):
    rows = pieces[0].shape[1]

    @pl.when(pl.program_id(0) == 0)
    def _():
        slot = 0
        for piece in pieces:
            for part in range(piece.shape[0]):
                start = pl.multiple_of(place_ref[slot] * rows, rows)
                columns_ref[pl.ds(start, rows), :] = piece[part]
                slot += 1


def tile_product(tiles, columns_ref):
    tile = jnp.concatenate([ref[0] for ref in tiles], axis=0)
    out = jnp.dot(tile, columns_ref[...], preferred_element_type=jnp.float32)
    return out.reshape(GROUP, -1, out.shape[1])


def given_kernel(order_ref, place_ref, *refs):
    tiles, (*pieces, out_ref, columns_ref) = refs[:GROUP], refs[GROUP:]
    fill_columns(place_ref, pieces, columns_ref)
    out_ref[...] = tile_product(tiles, columns_ref).astype(out_ref.dtype)


def mine_kernel(order_ref, place_ref, *refs):
    tiles, (*pieces, other_ref, o0, o1, o2, o3, columns_ref) = refs[:GROUP], refs[GROUP:]
    fill_columns(place_ref, pieces, columns_ref)
    both = tile_product(tiles, columns_ref) + other_ref[...].astype(jnp.float32)
    for d, out_ref in enumerate((o0, o1, o2, o3)):

        @pl.when(pl.program_id(0) == d)
        def _(out_ref=out_ref):
            out_ref[...] = both.astype(out_ref.dtype)


def product(tile, pieces, order, place, other=None):
    blocks = order.shape[0]
    _, rows, depth = tile.shape
    width = pieces[0].shape[2]

    def tile_spec(member):
        return pl.BlockSpec(
            (1, rows, depth), lambda i, order, place: (order[GROUP * i + member], 0, 0)
        )

    whole = lambda i, order, place: (0, 0, 0)
    step = pl.BlockSpec((GROUP, rows, width), lambda i, order, place: (i, 0, 0))
    in_specs = [tile_spec(member) for member in range(GROUP)]
    in_specs += [pl.BlockSpec(p.shape, whole) for p in pieces]
    operands = [tile] * GROUP + list(pieces)
    if other is None:
        kernel, out_specs = given_kernel, step
        out_shape = jax.ShapeDtypeStruct((blocks, rows, width), jnp.bfloat16)
    else:
        kernel, out_specs = mine_kernel, [pl.BlockSpec((GROUP, rows, width), whole)] * 4
        out_shape = [
            jax.ShapeDtypeStruct((GROUP, rows, width), dtype)
            for dtype in (jnp.float32, jnp.bfloat16, jnp.bfloat16, jnp.bfloat16)
        ]
        in_specs.append(step)
        operands.append(other)
    return pl.pallas_call(
        kernel,
        out_shape=out_shape,
        grid_spec=pltpu.PrefetchScalarGridSpec(
            num_scalar_prefetch=2,
            grid=(blocks // GROUP,),
            in_specs=in_specs,
            out_specs=out_specs,
            scratch_shapes=[pltpu.VMEM((depth, width), jnp.bfloat16)],
        ),
        compiler_params=pltpu.CompilerParams(vmem_limit_bytes=40 * 2**20),
        cost_estimate=pl.CostEstimate(
            flops=2 * blocks * rows * depth * width,
            bytes_accessed=2 * blocks * rows * depth + 2 * depth * width,
            transcendentals=0,
        ),
        name="product",
    )(order, place, *operands)


def total(term):
    core = lax.axis_index("core")
    half = term.shape[0] // 2
    chips = 64
    low, high = term[:half], term[half:]
    part = jnp.where(core == 0, low, high) + shift(jnp.where(core == 0, high, low), core=1)
    slices = part.astype(jnp.bfloat16).reshape(chips, half // chips, -1)
    slices = lax.all_to_all(slices, CHIPS, 0, 0)
    summed = jnp.sum(slices.astype(jnp.float32), axis=0, keepdims=True).astype(jnp.bfloat16)
    spread = lax.all_to_all(jnp.broadcast_to(summed, slices.shape), CHIPS, 0, 0)
    own = spread.reshape(half, -1)
    other = shift(own, core=1)
    return jnp.concatenate([jnp.where(core == 0, own, other), jnp.where(core == 0, other, own)])


def invert(diag_blocks, pivot_flags, panels, structure, ancestor_inverse):
    nodes, own_rows, _ = panels.shape
    z_hi, x, z_lo, y, core = [lax.axis_index(name) for name in AXES]
    tile = ancestor_inverse.reshape(16, own_rows, ancestor_inverse.shape[1])
    masked = [
        jnp.where(structure[k][:, None] != 0, panels[k], 0).astype(jnp.bfloat16)
        for k in range(nodes)
    ]
    steps = [(d, e) for d in range(4) for e in range(2)]
    kept = jnp.stack([(z_lo ^ e) * 8 + (y + d) % 4 * 2 + core for d, e in steps]).astype(jnp.int32)

    seeds = []
    for flip in range(2):
        seeds.append(seed(masked[0], flip))
    crossed = send(
        masked[1], lambda z_hi, x, z_lo, y, core: dict(z_hi=z_lo, z_lo=z_hi)
    )
    along = [crossed]
    for d in (1, 2, 3):
        along.append(shift(crossed, x=d))

    state = eliminate(0, diag_blocks, pivot_flags)

    pair = after(jnp.stack(seeds), state)
    first = [pair]
    for d in (1, 2, 3):
        first.append(shift(pair, x=d))
    first_place = jnp.stack([(z_hi ^ e) * 4 + (x - d) % 4 for d, e in steps]).astype(jnp.int32)

    state = eliminate(1, after(state, pair), pivot_flags)
    stacked = after(jnp.stack(along), state)
    turned = []
    for d in range(4):
        part = lax.dynamic_index_in_dim(stacked, (x - y - d) % 4, 0, keepdims=False)
        turned.append(shift(part, y=d) if d else part)

    state = eliminate(2, after(state, stacked), pivot_flags)
    quad = after(jnp.stack(turned), state)
    second = []
    for flip in range(2):
        second.append(
            send(
                quad,
                lambda z_hi, x, z_lo, y, core: dict(z_hi=core ^ flip, core=z_hi),
            )
        )
    second_place = jnp.stack(
        [(y - d) % 4 * 2 + (z_hi ^ flip) for flip in range(2) for d in range(4)]
    ).astype(jnp.int32)

    pieces = [first, second]
    places = [first_place, second_place]
    sums = []
    order = after(kept, quad)
    for k in range(nodes):
        given = product(tile, pieces[k], order ^ 1, places[k])
        other = shift(given, core=1)
        staying, *leaving = product(tile, pieces[k], order, places[k], other)
        order = after(kept, *leaving)
        summed = staying
        for d, part in zip((1, 2, 3), leaving):
            arrived = shift(part, y=d)
            summed = summed + arrived.astype(jnp.float32)
        arrived = shift(summed[1].astype(jnp.bfloat16), z_lo=1)
        sums.append(summed[0] + arrived.astype(jnp.float32))

    inverses = eliminate(3, after(state, *leaving), pivot_flags)
    applied, terms = [], []
    for k in range(nodes):
        applied.append(jnp.dot(sums[k], inverses[k], precision=HIGHEST))
        normed = jnp.dot(masked[k].astype(jnp.float32), inverses[k], precision=HIGHEST)
        terms.append(
            lax.dot_general(
                normed.astype(jnp.bfloat16).astype(jnp.float32),
                applied[k],
                (((0,), (0,)), ((), ())),
                precision=HIGHEST,
                preferred_element_type=jnp.float32,
            )
        )
    totals = total(jnp.concatenate(terms)).astype(jnp.float32).reshape(inverses.shape)
    inverse_diagonal = inverses + totals
    inverse_panel = (-jnp.stack(applied)).astype(jnp.bfloat16)
    return (inverse_panel, inverse_diagonal)


def solution(mesh):
    mesh = Mesh(mesh.devices.reshape(MESH_SHAPE), AXES)
    in_specs = (P(), P(), P(None, AXES, None), P(None, AXES), P(ROW, COL))
    out_specs = (P(None, AXES, None), P())
    return jax.shard_map(invert, mesh=mesh, in_specs=in_specs, out_specs=out_specs, check_vma=False)
```

```python
import functools

import jax
import jax.numpy as jnp
import numpy as np
from jax import lax
from jax.experimental import pallas as pl
from jax.experimental.pallas import tpu as pltpu
from jax.sharding import Mesh, PartitionSpec as P

HIGHEST = lax.Precision.HIGHEST
PERTURBATION = 1.0
BLOCK = 128
STRIP = 8
GROUP = 2
ROW = ("z_hi", "x")
COL = ("z_lo", "y", "core")
AXES = ROW + COL
CHIPS = ("z_hi", "x", "z_lo", "y")
MESH_SHAPE = (2, 4, 2, 4, 2)


def after(value, *earlier):
    return lax.optimization_barrier((value, earlier))[0]


def lane_spread(tile, lane):
    index = jnp.full(tile.shape, lane, jnp.int32)
    return jnp.take_along_axis(tile, index, axis=1, mode="promise_in_bounds")


def small_inverses(nodes):
    row = lax.broadcasted_iota(jnp.int32, nodes[0][0].shape, 0)
    for i in range(len(nodes[0])):
        at = row == i
        pivot = [1.0 / cols[i][i : i + 1, :] for cols in nodes]
        left = [jnp.where(at, -1.0, cols[i]) for cols in nodes]
        nodes = [
            [
                -l * p if j == i else jnp.where(at, 0.0, cols[j]) - l * (cols[j][i : i + 1, :] * p)
                for j in range(len(cols))
            ]
            for cols, l, p in zip(nodes, left, pivot)
        ]
    return nodes


def invert_blocks(ref):
    count, n, _ = ref.shape
    nodes = range(count)
    lane = lax.broadcasted_iota(jnp.int32, (STRIP, n), 1)
    wide = lax.broadcasted_iota(jnp.int32, (n, n), 1)

    def step(strip, carry):
        base = pl.multiple_of(strip * STRIP, STRIP)
        inside = (wide >= base) & (wide < base + STRIP)
        whole = [ref[k] for k in nodes]
        rows = [ref[k, pl.ds(base, STRIP), :] for k in nodes]
        small = small_inverses(
            [[lane_spread(rows[k], base + j) for j in range(STRIP)] for k in nodes]
        )
        top = [small[k][0] * rows[k][0:1, :] for k in nodes]
        for j in range(1, STRIP):
            top = [top[k] + small[k][j] * rows[k][j : j + 1, :] for k in nodes]
        for j in range(STRIP):
            top = [jnp.where(lane == base + j, small[k][j], top[k]) for k in nodes]
        rest = [jnp.where(inside, 0.0, whole[k]) for k in nodes]
        for j in range(STRIP):
            rest = [
                rest[k] - lane_spread(whole[k], base + j) * top[k][j : j + 1, :] for k in nodes
            ]
        for k in nodes:
            ref[k] = rest[k]
            ref[k, pl.ds(base, STRIP), :] = top[k]
        return carry

    lax.fori_loop(0, n // STRIP, step, 0)


def split_dot(a, b):
    a_head, b_head = a.astype(jnp.bfloat16), b.astype(jnp.bfloat16)
    a_rest = (a - a_head.astype(jnp.float32)).astype(jnp.bfloat16)
    b_rest = (b - b_head.astype(jnp.float32)).astype(jnp.bfloat16)
    dot = functools.partial(jnp.dot, preferred_element_type=jnp.float32)
    return dot(a_head, b_head) + (dot(a_head, b_rest) + dot(a_rest, b_head))


def inverse_kernel(block, in_ref, flag_ref, out_ref, block_ref, panel_ref):
    count, width, _ = in_ref.shape
    n = block_ref.shape[1]
    here = pl.ds(block * n, n)
    if block == 0:
        row = lax.broadcasted_iota(jnp.int32, (width, width), 0)
        col = lax.broadcasted_iota(jnp.int32, (width, width), 1)
        for k in range(count):
            shifts = PERTURBATION * flag_ref[k : k + 1, :].astype(jnp.float32)
            out_ref[k] = in_ref[k] + jnp.where(row == col, shifts, 0.0)
    else:
        out_ref[...] = in_ref[...]
    for k in range(count):
        block_ref[k] = out_ref[k, here, here]
    invert_blocks(block_ref)

    def update(k, carry):
        inner = block_ref[k]
        panel_ref[...] = split_dot(inner, out_ref[k, here, :])
        panel_ref[:, here] = inner
        left = out_ref[k, :, here]
        out_ref[k, :, here] = jnp.zeros((width, n), jnp.float32)
        out_ref[k] = out_ref[k] - split_dot(left, panel_ref[...])
        out_ref[k, here, :] = panel_ref[...]
        return carry

    lax.fori_loop(0, count, update, 0)


def eliminate(block, matrices, pivot_flags):
    count, width, _ = matrices.shape
    return pl.pallas_call(
        functools.partial(inverse_kernel, block),
        out_shape=jax.ShapeDtypeStruct(matrices.shape, jnp.float32),
        scratch_shapes=[
            pltpu.VMEM((count, BLOCK, BLOCK), jnp.float32),
            pltpu.VMEM((BLOCK, width), jnp.float32),
        ],
        compiler_params=pltpu.CompilerParams(vmem_limit_bytes=32 * 2**20),
        cost_estimate=pl.CostEstimate(
            flops=5 * 10**9, bytes_accessed=8 * matrices.size, transcendentals=0
        ),
        name="eliminate",
    )(matrices, pivot_flags)


def shift(value, **steps):
    return send(value, lambda **at: {name: at[name] + by for name, by in steps.items()})


def send(value, target):
    extents = [lax.axis_size(name) for name in AXES]
    moves = []
    for source in np.ndindex(*extents):
        at = {name: int(i) for name, i in zip(AXES, source)}
        at.update(target(**at))
        there = [at[name] % extent for name, extent in zip(AXES, extents)]
        moves.append(tuple(int(np.ravel_multi_index(i, extents)) for i in (source, there)))
    return lax.ppermute(value, AXES, moves)


def seed(strip, flip):
    return send(
        strip,
        lambda z_hi, x, z_lo, y, core: dict(
            z_hi=y // 2 ^ flip, x=y % 2 * 2 + core, z_lo=z_hi, y=x, core=z_lo
        ),
    )


def fill_columns(place_ref, pieces, columns_ref):
    rows = pieces[0].shape[1]

    @pl.when(pl.program_id(0) == 0)
    def _():
        slot = 0
        for piece in pieces:
            for part in range(piece.shape[0]):
                start = pl.multiple_of(place_ref[slot] * rows, rows)
                columns_ref[pl.ds(start, rows), :] = piece[part]
                slot += 1


def tile_product(tiles, columns_ref):
    tile = jnp.concatenate([ref[0] for ref in tiles], axis=0)
    out = jnp.dot(tile, columns_ref[...], preferred_element_type=jnp.float32)
    return out.reshape(GROUP, -1, out.shape[1])


def given_kernel(order_ref, place_ref, *refs):
    tiles, (*pieces, out_ref, columns_ref) = refs[:GROUP], refs[GROUP:]
    fill_columns(place_ref, pieces, columns_ref)
    out_ref[...] = tile_product(tiles, columns_ref).astype(out_ref.dtype)


def mine_kernel(order_ref, place_ref, *refs):
    tiles, (*pieces, other_ref, o0, o1, o2, o3, columns_ref) = refs[:GROUP], refs[GROUP:]
    fill_columns(place_ref, pieces, columns_ref)
    both = tile_product(tiles, columns_ref) + other_ref[...].astype(jnp.float32)
    for d, out_ref in enumerate((o0, o1, o2, o3)):

        @pl.when(pl.program_id(0) == d)
        def _(out_ref=out_ref):
            out_ref[...] = both.astype(out_ref.dtype)


def product(tile, pieces, order, place, other=None):
    blocks = order.shape[0]
    _, rows, depth = tile.shape
    width = pieces[0].shape[2]

    def tile_spec(member):
        return pl.BlockSpec(
            (1, rows, depth), lambda i, order, place: (order[GROUP * i + member], 0, 0)
        )

    whole = lambda i, order, place: (0, 0, 0)
    step = pl.BlockSpec((GROUP, rows, width), lambda i, order, place: (i, 0, 0))
    in_specs = [tile_spec(member) for member in range(GROUP)]
    in_specs += [pl.BlockSpec(p.shape, whole) for p in pieces]
    operands = [tile] * GROUP + list(pieces)
    if other is None:
        kernel, out_specs = given_kernel, step
        out_shape = jax.ShapeDtypeStruct((blocks, rows, width), jnp.bfloat16)
    else:
        kernel, out_specs = mine_kernel, [pl.BlockSpec((GROUP, rows, width), whole)] * 4
        out_shape = [
            jax.ShapeDtypeStruct((GROUP, rows, width), dtype)
            for dtype in (jnp.float32, jnp.bfloat16, jnp.bfloat16, jnp.bfloat16)
        ]
        in_specs.append(step)
        operands.append(other)
    return pl.pallas_call(
        kernel,
        out_shape=out_shape,
        grid_spec=pltpu.PrefetchScalarGridSpec(
            num_scalar_prefetch=2,
            grid=(blocks // GROUP,),
            in_specs=in_specs,
            out_specs=out_specs,
            scratch_shapes=[pltpu.VMEM((depth, width), jnp.bfloat16)],
        ),
        compiler_params=pltpu.CompilerParams(vmem_limit_bytes=40 * 2**20),
        cost_estimate=pl.CostEstimate(
            flops=2 * blocks * rows * depth * width,
            bytes_accessed=2 * blocks * rows * depth + 2 * depth * width,
            transcendentals=0,
        ),
        name="product",
    )(order, place, *operands)


def total(term):
    core = lax.axis_index("core")
    half = term.shape[0] // 2
    chips = 64
    low, high = term[:half], term[half:]
    part = jnp.where(core == 0, low, high) + shift(jnp.where(core == 0, high, low), core=1)
    slices = part.astype(jnp.bfloat16).reshape(chips, half // chips, -1)
    slices = lax.all_to_all(slices, CHIPS, 0, 0)
    summed = jnp.sum(slices.astype(jnp.float32), axis=0, keepdims=True).astype(jnp.bfloat16)
    spread = lax.all_to_all(jnp.broadcast_to(summed, slices.shape), CHIPS, 0, 0)
    own = spread.reshape(half, -1)
    other = shift(own, core=1)
    return jnp.concatenate([jnp.where(core == 0, own, other), jnp.where(core == 0, other, own)])


def invert(diag_blocks, pivot_flags, panels, structure, ancestor_inverse):
    nodes, own_rows, _ = panels.shape
    z_hi, x, z_lo, y, core = [lax.axis_index(name) for name in AXES]
    tile = ancestor_inverse.reshape(16, own_rows, ancestor_inverse.shape[1])
    masked = [
        jnp.where(structure[k][:, None] != 0, panels[k], 0).astype(jnp.bfloat16)
        for k in range(nodes)
    ]
    steps = [(d, e) for d in range(4) for e in range(2)]
    kept = jnp.stack([(z_lo ^ e) * 8 + (y + d) % 4 * 2 + core for d, e in steps]).astype(jnp.int32)

    seeds = []
    for flip in range(2):
        seeds.append(seed(masked[0], flip))
    crossed = send(
        masked[1], lambda z_hi, x, z_lo, y, core: dict(z_hi=z_lo, z_lo=z_hi)
    )
    along = [crossed]
    for d in (1, 2, 3):
        along.append(shift(crossed, x=d))

    state = eliminate(0, diag_blocks, pivot_flags)

    pair = after(jnp.stack(seeds), state)
    first = [pair]
    for d in (1, 2, 3):
        first.append(shift(pair, x=d))
    first_place = jnp.stack([(z_hi ^ e) * 4 + (x - d) % 4 for d, e in steps]).astype(jnp.int32)

    stacked = after(jnp.stack(along), pair)
    turned = []
    for d in range(4):
        part = lax.dynamic_index_in_dim(stacked, (x - y - d) % 4, 0, keepdims=False)
        turned.append(shift(part, y=d) if d else part)

    quad = jnp.stack(turned)
    second = []
    for flip in range(2):
        second.append(
            send(
                quad,
                lambda z_hi, x, z_lo, y, core: dict(z_hi=core ^ flip, core=z_hi),
            )
        )
    second_place = jnp.stack(
        [(y - d) % 4 * 2 + (z_hi ^ flip) for flip in range(2) for d in range(4)]
    ).astype(jnp.int32)

    pieces = [first, second]
    places = [first_place, second_place]
    sums = []
    order = after(kept, quad)
    for k in range(nodes):
        given = product(tile, pieces[k], order ^ 1, places[k])
        other = shift(given, core=1)
        if k == 0:
            state = eliminate(1, after(state, given), pivot_flags)
        staying, *leaving = product(tile, pieces[k], order, places[k], other)
        order = after(kept, *leaving)
        summed = staying
        for d, part in zip((1, 2, 3), leaving):
            arrived = shift(part, y=d)
            summed = summed + arrived.astype(jnp.float32)
        arrived = shift(summed[1].astype(jnp.bfloat16), z_lo=1)
        sums.append(summed[0] + arrived.astype(jnp.float32))

    state = eliminate(2, after(state, *leaving), pivot_flags)
    inverses = eliminate(3, state, pivot_flags)
    applied, terms = [], []
    for k in range(nodes):
        applied.append(jnp.dot(sums[k], inverses[k], precision=HIGHEST))
        normed = jnp.dot(masked[k].astype(jnp.float32), inverses[k], precision=HIGHEST)
        terms.append(
            lax.dot_general(
                normed.astype(jnp.bfloat16).astype(jnp.float32),
                applied[k],
                (((0,), (0,)), ((), ())),
                precision=HIGHEST,
                preferred_element_type=jnp.float32,
            )
        )
    totals = total(jnp.concatenate(terms)).astype(jnp.float32).reshape(inverses.shape)
    inverse_diagonal = inverses + totals
    inverse_panel = (-jnp.stack(applied)).astype(jnp.bfloat16)
    return (inverse_panel, inverse_diagonal)


def solution(mesh):
    mesh = Mesh(mesh.devices.reshape(MESH_SHAPE), AXES)
    in_specs = (P(), P(), P(None, AXES, None), P(None, AXES), P(ROW, COL))
    out_specs = (P(None, AXES, None), P())
    return jax.shard_map(invert, mesh=mesh, in_specs=in_specs, out_specs=out_specs, check_vma=False)
```

```python
import functools

import jax
import jax.numpy as jnp
import numpy as np
from jax import lax
from jax.experimental import pallas as pl
from jax.experimental.pallas import tpu as pltpu
from jax.sharding import Mesh, PartitionSpec as P

HIGHEST = lax.Precision.HIGHEST
PERTURBATION = 1.0
BLOCK = 128
STRIP = 8
GROUP = 2
ROW = ("z_hi", "x")
COL = ("z_lo", "y", "core")
AXES = ROW + COL
CHIPS = ("z_hi", "x", "z_lo", "y")
MESH_SHAPE = (2, 4, 2, 4, 2)


def after(value, *earlier):
    return lax.optimization_barrier((value, earlier))[0]


def lane_spread(tile, lane):
    index = jnp.full(tile.shape, lane, jnp.int32)
    return jnp.take_along_axis(tile, index, axis=1, mode="promise_in_bounds")


def small_inverses(nodes):
    row = lax.broadcasted_iota(jnp.int32, nodes[0][0].shape, 0)
    for i in range(len(nodes[0])):
        at = row == i
        pivot = [1.0 / cols[i][i : i + 1, :] for cols in nodes]
        left = [jnp.where(at, -1.0, cols[i]) for cols in nodes]
        nodes = [
            [
                -l * p if j == i else jnp.where(at, 0.0, cols[j]) - l * (cols[j][i : i + 1, :] * p)
                for j in range(len(cols))
            ]
            for cols, l, p in zip(nodes, left, pivot)
        ]
    return nodes


def invert_blocks(ref):
    count, n, _ = ref.shape
    nodes = range(count)
    lane = lax.broadcasted_iota(jnp.int32, (STRIP, n), 1)
    wide = lax.broadcasted_iota(jnp.int32, (n, n), 1)

    def step(strip, carry):
        base = pl.multiple_of(strip * STRIP, STRIP)
        inside = (wide >= base) & (wide < base + STRIP)
        whole = [ref[k] for k in nodes]
        rows = [ref[k, pl.ds(base, STRIP), :] for k in nodes]
        small = small_inverses(
            [[lane_spread(rows[k], base + j) for j in range(STRIP)] for k in nodes]
        )
        top = [small[k][0] * rows[k][0:1, :] for k in nodes]
        for j in range(1, STRIP):
            top = [top[k] + small[k][j] * rows[k][j : j + 1, :] for k in nodes]
        for j in range(STRIP):
            top = [jnp.where(lane == base + j, small[k][j], top[k]) for k in nodes]
        rest = [jnp.where(inside, 0.0, whole[k]) for k in nodes]
        for j in range(STRIP):
            rest = [
                rest[k] - lane_spread(whole[k], base + j) * top[k][j : j + 1, :] for k in nodes
            ]
        for k in nodes:
            ref[k] = rest[k]
            ref[k, pl.ds(base, STRIP), :] = top[k]
        return carry

    lax.fori_loop(0, n // STRIP, step, 0)


def split_dot(a, b):
    a_head, b_head = a.astype(jnp.bfloat16), b.astype(jnp.bfloat16)
    a_rest = (a - a_head.astype(jnp.float32)).astype(jnp.bfloat16)
    b_rest = (b - b_head.astype(jnp.float32)).astype(jnp.bfloat16)
    dot = functools.partial(jnp.dot, preferred_element_type=jnp.float32)
    return dot(a_head, b_head) + (dot(a_head, b_rest) + dot(a_rest, b_head))


def inverse_kernel(block, in_ref, flag_ref, out_ref, block_ref, panel_ref):
    count, width, _ = in_ref.shape
    n = block_ref.shape[1]
    here = pl.ds(block * n, n)
    if block == 0:
        row = lax.broadcasted_iota(jnp.int32, (width, width), 0)
        col = lax.broadcasted_iota(jnp.int32, (width, width), 1)
        for k in range(count):
            shifts = PERTURBATION * flag_ref[k : k + 1, :].astype(jnp.float32)
            out_ref[k] = in_ref[k] + jnp.where(row == col, shifts, 0.0)
    else:
        out_ref[...] = in_ref[...]
    for k in range(count):
        block_ref[k] = out_ref[k, here, here]
    invert_blocks(block_ref)

    def update(k, carry):
        inner = block_ref[k]
        panel_ref[...] = split_dot(inner, out_ref[k, here, :])
        panel_ref[:, here] = inner
        left = out_ref[k, :, here]
        out_ref[k, :, here] = jnp.zeros((width, n), jnp.float32)
        out_ref[k] = out_ref[k] - split_dot(left, panel_ref[...])
        out_ref[k, here, :] = panel_ref[...]
        return carry

    lax.fori_loop(0, count, update, 0)


def eliminate(block, matrices, pivot_flags):
    count, width, _ = matrices.shape
    return pl.pallas_call(
        functools.partial(inverse_kernel, block),
        out_shape=jax.ShapeDtypeStruct(matrices.shape, jnp.float32),
        scratch_shapes=[
            pltpu.VMEM((count, BLOCK, BLOCK), jnp.float32),
            pltpu.VMEM((BLOCK, width), jnp.float32),
        ],
        compiler_params=pltpu.CompilerParams(vmem_limit_bytes=32 * 2**20),
        cost_estimate=pl.CostEstimate(
            flops=5 * 10**9, bytes_accessed=8 * matrices.size, transcendentals=0
        ),
        name="eliminate",
    )(matrices, pivot_flags)


def shift(value, **steps):
    return send(value, lambda **at: {name: at[name] + by for name, by in steps.items()})


def send(value, target):
    extents = [lax.axis_size(name) for name in AXES]
    moves = []
    for source in np.ndindex(*extents):
        at = {name: int(i) for name, i in zip(AXES, source)}
        at.update(target(**at))
        there = [at[name] % extent for name, extent in zip(AXES, extents)]
        moves.append(tuple(int(np.ravel_multi_index(i, extents)) for i in (source, there)))
    return lax.ppermute(value, AXES, moves)


def seed(strip, flip):
    return send(
        strip,
        lambda z_hi, x, z_lo, y, core: dict(
            z_hi=y // 2 ^ flip, x=y % 2 * 2 + core, z_lo=z_hi, y=x, core=z_lo
        ),
    )


def fill_columns(place_ref, pieces, columns_ref):
    rows = pieces[0].shape[1]

    @pl.when(pl.program_id(0) == 0)
    def _():
        slot = 0
        for piece in pieces:
            for part in range(piece.shape[0]):
                start = pl.multiple_of(place_ref[slot] * rows, rows)
                columns_ref[pl.ds(start, rows), :] = piece[part]
                slot += 1


def tile_product(tiles, columns_ref):
    tile = jnp.concatenate([ref[0] for ref in tiles], axis=0)
    out = jnp.dot(tile, columns_ref[...], preferred_element_type=jnp.float32)
    return out.reshape(GROUP, -1, out.shape[1])


def given_kernel(order_ref, place_ref, *refs):
    tiles, (*pieces, out_ref, columns_ref) = refs[:GROUP], refs[GROUP:]
    fill_columns(place_ref, pieces, columns_ref)
    out_ref[...] = tile_product(tiles, columns_ref).astype(out_ref.dtype)


def mine_kernel(order_ref, place_ref, *refs):
    tiles, (*pieces, other_ref, o0, o1, o2, o3, columns_ref) = refs[:GROUP], refs[GROUP:]
    fill_columns(place_ref, pieces, columns_ref)
    both = tile_product(tiles, columns_ref) + other_ref[...].astype(jnp.float32)
    for d, out_ref in enumerate((o0, o1, o2, o3)):

        @pl.when(pl.program_id(0) == d)
        def _(out_ref=out_ref):
            out_ref[...] = both.astype(out_ref.dtype)


def product(tile, pieces, order, place, other=None):
    blocks = order.shape[0]
    _, rows, depth = tile.shape
    width = pieces[0].shape[2]

    def tile_spec(member):
        return pl.BlockSpec(
            (1, rows, depth), lambda i, order, place: (order[GROUP * i + member], 0, 0)
        )

    whole = lambda i, order, place: (0, 0, 0)
    step = pl.BlockSpec((GROUP, rows, width), lambda i, order, place: (i, 0, 0))
    in_specs = [tile_spec(member) for member in range(GROUP)]
    in_specs += [pl.BlockSpec(p.shape, whole) for p in pieces]
    operands = [tile] * GROUP + list(pieces)
    if other is None:
        kernel, out_specs = given_kernel, step
        out_shape = jax.ShapeDtypeStruct((blocks, rows, width), jnp.bfloat16)
    else:
        kernel, out_specs = mine_kernel, [pl.BlockSpec((GROUP, rows, width), whole)] * 4
        out_shape = [
            jax.ShapeDtypeStruct((GROUP, rows, width), dtype)
            for dtype in (jnp.float32, jnp.bfloat16, jnp.bfloat16, jnp.bfloat16)
        ]
        in_specs.append(step)
        operands.append(other)
    return pl.pallas_call(
        kernel,
        out_shape=out_shape,
        grid_spec=pltpu.PrefetchScalarGridSpec(
            num_scalar_prefetch=2,
            grid=(blocks // GROUP,),
            in_specs=in_specs,
            out_specs=out_specs,
            scratch_shapes=[pltpu.VMEM((depth, width), jnp.bfloat16)],
        ),
        compiler_params=pltpu.CompilerParams(vmem_limit_bytes=40 * 2**20),
        cost_estimate=pl.CostEstimate(
            flops=2 * blocks * rows * depth * width,
            bytes_accessed=2 * blocks * rows * depth + 2 * depth * width,
            transcendentals=0,
        ),
        name="product",
    )(order, place, *operands)


def total(term):
    core = lax.axis_index("core")
    half = term.shape[0] // 2
    chips = 64
    low, high = term[:half], term[half:]
    part = jnp.where(core == 0, low, high) + shift(jnp.where(core == 0, high, low), core=1)
    slices = part.astype(jnp.bfloat16).reshape(chips, half // chips, -1)
    slices = lax.all_to_all(slices, CHIPS, 0, 0)
    summed = jnp.sum(slices.astype(jnp.float32), axis=0, keepdims=True).astype(jnp.bfloat16)
    spread = lax.all_to_all(jnp.broadcast_to(summed, slices.shape), CHIPS, 0, 0)
    own = spread.reshape(half, -1)
    other = shift(own, core=1)
    return jnp.concatenate([jnp.where(core == 0, own, other), jnp.where(core == 0, other, own)])


def invert(diag_blocks, pivot_flags, panels, structure, ancestor_inverse):
    nodes, own_rows, _ = panels.shape
    z_hi, x, z_lo, y, core = [lax.axis_index(name) for name in AXES]
    tile = ancestor_inverse.reshape(16, own_rows, ancestor_inverse.shape[1])
    masked = [
        jnp.where(structure[k][:, None] != 0, panels[k], 0).astype(jnp.bfloat16)
        for k in range(nodes)
    ]
    steps = [(d, e) for d in range(4) for e in range(2)]
    kept = jnp.stack([(z_lo ^ e) * 8 + (y + d) % 4 * 2 + core for d, e in steps]).astype(jnp.int32)

    seeds = []
    for flip in range(2):
        seeds.append(seed(masked[0], flip))
    crossed = send(
        masked[1], lambda z_hi, x, z_lo, y, core: dict(z_hi=z_lo, z_lo=z_hi)
    )
    along = [crossed]
    for d in (1, 2, 3):
        along.append(shift(crossed, x=d))

    state = eliminate(0, diag_blocks, pivot_flags)

    pair = after(jnp.stack(seeds), state)
    first = [pair]
    for d in (1, 2, 3):
        first.append(shift(pair, x=d))
    first_place = jnp.stack([(z_hi ^ e) * 4 + (x - d) % 4 for d, e in steps]).astype(jnp.int32)

    stacked = after(jnp.stack(along), pair)
    turned = []
    for d in range(4):
        part = lax.dynamic_index_in_dim(stacked, (x - y - d) % 4, 0, keepdims=False)
        turned.append(shift(part, y=d) if d else part)

    quad = jnp.stack(turned)
    second = []
    for flip in range(2):
        second.append(
            send(
                quad,
                lambda z_hi, x, z_lo, y, core: dict(z_hi=core ^ flip, core=z_hi),
            )
        )
    second_place = jnp.stack(
        [(y - d) % 4 * 2 + (z_hi ^ flip) for flip in range(2) for d in range(4)]
    ).astype(jnp.int32)

    pieces = [first, second]
    places = [first_place, second_place]
    sums = []
    order = after(kept, quad)
    for k in range(nodes):
        given = product(tile, pieces[k], order ^ 1, places[k])
        other = shift(given, core=1)
        if k == 0:
            state = eliminate(1, after(state, given), pivot_flags)
        staying, *leaving = product(tile, pieces[k], order, places[k], other)
        order = after(kept, *leaving)
        summed = staying
        for d, part in zip((1, 2, 3), leaving):
            arrived = shift(part, y=d)
            summed = summed + arrived.astype(jnp.float32)
        rising = summed[1].astype(jnp.bfloat16)
        arrived = shift(rising, z_lo=1)
        sums.append(summed[0] + arrived.astype(jnp.float32))

    state = eliminate(2, after(state, *leaving), pivot_flags)
    inverses = eliminate(3, state, pivot_flags)
    ready = after(inverses, rising)
    applied, terms = [], []
    for k in range(nodes):
        applied.append(jnp.dot(sums[k], ready[k], precision=HIGHEST))
        normed = jnp.dot(masked[k].astype(jnp.float32), ready[k], precision=HIGHEST)
        terms.append(
            lax.dot_general(
                normed.astype(jnp.bfloat16).astype(jnp.float32),
                applied[k],
                (((0,), (0,)), ((), ())),
                precision=HIGHEST,
                preferred_element_type=jnp.float32,
            )
        )
    totals = total(jnp.concatenate(terms)).astype(jnp.float32).reshape(inverses.shape)
    inverse_diagonal = inverses + totals
    inverse_panel = (-jnp.stack(applied)).astype(jnp.bfloat16)
    return (inverse_panel, inverse_diagonal)


def solution(mesh):
    mesh = Mesh(mesh.devices.reshape(MESH_SHAPE), AXES)
    in_specs = (P(), P(), P(None, AXES, None), P(None, AXES), P(ROW, COL))
    out_specs = (P(None, AXES, None), P())
    return jax.shard_map(invert, mesh=mesh, in_specs=in_specs, out_specs=out_specs, check_vma=False)
```
